32 devices in a mesh: section: 4 (over y, x), owner: 8 (over z, core).
Axes of the slice: x: 2, y: 2, z: 4, core: 2. Of those that a mesh axis runs over, the one named last changes fastest.
Arguments:
- weights: bfloat16 [4, 1024, 1024], P('section'), may hold values from -0.1875 to 0.1875
- inputs: bfloat16 [4, 4, 2048, 1024], P('section', None, 'owner'), may hold values from -6 to 6
- preact: bfloat16 [4, 4, 2048, 1024], P('section', None, 'owner'), may hold values from -6 to 6
- cotangent: bfloat16 [4, 2048, 1024], P(None, 'owner'), may hold values from -6 to 6
- embeddings: bfloat16 [4, 2048, 32, 128], P(None, ('owner', 'section')), may hold values from -6 to 6
- row_ids: int32 [4, 2048, 32], P(None, ('owner', 'section')), may hold values from 0 to 511
Outputs:
- weight_grad: float32 [4, 1024, 1024], P('section', 'owner')
- table_grad: float32 [32, 512, 128], P('owner', 'section')
The draws below stay inside these ranges and needn't reach their ends.
All inputs are finite; a program needn't handle non-finite values.
Results may differ from the reference program's by a relative error of at most 0.0064.
Values may be sent and summed in bfloat16 or wider, within the bound.
A program may use at most 128 MiB of HBM per device.

```python
import math
import jax
import jax.numpy as jnp
import numpy as np
from jax import lax

F = 32
E = 128
H = 1024
MICRO = 4
TROWS = 512
LAYERS = 4
SLOTS = 32
ROWS = 512
BATCH = 2048


def with_ends(values, own_key, low, high):
    longest = values.shape.index(max(values.shape))
    spots = []
    for shift in (0, 1):
        where = [jax.random.randint(jax.random.fold_in(own_key, axis), (), 0, length) for axis, length in enumerate(values.shape)]
        where[longest] = (where[longest] + shift) % values.shape[longest]
        spots.append(tuple(where))
    return values.at[spots[0]].set(low).at[spots[1]].set(high)


def spiked(drawn, key, source, target, blocks, factor):
    def block_of(dim):
        return (jnp.arange(drawn.shape[dim]) // (drawn.shape[dim] // blocks)).reshape((-1,) + (1,) * (drawn.ndim - 1 - dim))

    near = jax.random.permutation(key, blocks)[block_of(target)]
    other_side = (block_of(target) + blocks // 2) % blocks
    return jnp.where((block_of(source) == near) | (block_of(source) == other_side), factor * drawn, drawn)


def shard_levels(key, extent, split, least, top_value):
    loudness = 1.0
    for dim, shards_of in split:
        draws = jax.random.uniform(jax.random.fold_in(jax.random.fold_in(key, 6), dim), (shards_of,), jnp.float32, least / len(split), top_value / len(split))
        loudness = loudness * jnp.repeat(jnp.exp(draws), extent[dim] // shards_of).reshape((-1,) + (1,) * (len(extent) - 1 - dim))
    return loudness


def rank_bounds(amount, skew):
    weights = [(1 << 20) // math.isqrt(standing ** skew) + 1 for standing in range(1, amount + 1)]
    deviation = 1 + sum(weights) // (1 << 30)
    return np.cumsum(np.array([max(1, weight // deviation) for weight in weights]))


def skewed_ids(stream_key, dims, number_of, skew):
    listing = rank_bounds(number_of, skew)
    ticket = jax.random.randint(jax.random.fold_in(stream_key, 1), dims, 0, int(listing[number_of - 1]))
    grade = jnp.searchsorted(jnp.asarray(listing, jnp.int32), ticket, side="right")
    return jax.random.permutation(jax.random.fold_in(stream_key, 2), number_of)[grade].astype(jnp.int32)


def gaussian(key, extent, width, limit, pieces=(), held_as=jnp.bfloat16):
    drawn = width * jax.random.normal(key, extent, jnp.float32)
    if pieces:
        drawn = drawn * shard_levels(key, extent, pieces, -0.22, 0.18)
    return jnp.clip(drawn, -limit, limit).astype(held_as)


def gaussian_with(rng, extent, spread, limit, pieces, heavy, kind=jnp.bfloat16):
    values = spread * jax.random.normal(rng, extent, jnp.float32)
    if pieces:
        values = values * shard_levels(rng, extent, pieces, -0.22, 0.18)
    return jnp.clip(spiked(values, jax.random.fold_in(rng, 3), *heavy), -limit, limit).astype(kind)


def setup_inputs(seed: int = 0) -> dict:
    arg_keys = jax.random.split(jax.random.key(seed), 7)
    return {
        "weights": gaussian(arg_keys[0], (LAYERS, H, H), H ** -0.5, 0.1875, ((0, 4),)),
        "inputs": gaussian_with(arg_keys[1], (LAYERS, MICRO, BATCH, H), 1.0, 6.0, ((0, 4), (2, 8)), (2, 3, 8, 2.0)),
        "preact": gaussian(arg_keys[2], (LAYERS, MICRO, BATCH, H), 1.0, 6.0, ((0, 4), (2, 8))),
        "cotangent": gaussian(arg_keys[3], (MICRO, BATCH, H), 1.0, 6.0, ((1, 8),)),
        "embeddings": gaussian(arg_keys[4], (MICRO, BATCH, F, E), 1.0, 6.0, ((1, 32),)),
        "row_ids": with_ends(skewed_ids(arg_keys[5], (MICRO, BATCH, F), ROWS, 2), jax.random.fold_in(arg_keys[5], 3), 0, ROWS - 1).astype(jnp.int32),
    }


def reference(weights, inputs, preact, cotangent, embeddings, row_ids):
    highest = lax.Precision.HIGHEST
    micro_count, sample_rows, hidden = cotangent.shape
    features = embeddings.shape[2]
    emb_width = embeddings.shape[3]
    grad_scale = 1.0 / math.sqrt(micro_count * sample_rows)
    upstream = cotangent
    layer_grads = []
    for layer_index in range(LAYERS - 1, -1, -1):
        slope = jnp.where(preact[layer_index] > 0, upstream, jnp.zeros_like(upstream))
        slope = slope.reshape(micro_count * sample_rows, hidden)
        flat_in = inputs[layer_index].reshape(micro_count * sample_rows, hidden)
        layer_grads.append(jnp.dot(flat_in.T.astype(jnp.float32), slope.astype(jnp.float32), precision=highest) * grad_scale)
        upstream = jnp.dot(slope.astype(jnp.float32), weights[layer_index].T.astype(jnp.float32), precision=highest)
        upstream = upstream.astype(jnp.bfloat16).reshape(micro_count, sample_rows, hidden)
    weight_grad = jnp.stack(layer_grads[::-1])

    def feature_grads(members):
        flat_grad, embedded = members
        square = flat_grad.reshape(sample_rows, features, features).astype(jnp.float32)
        emb32 = embedded.astype(jnp.float32)
        direct = jnp.einsum('qfg,qge->qfe', square, emb32, precision=highest)
        swapped = jnp.einsum('qgf,qge->qfe', square, emb32, precision=highest)
        return (direct + swapped).astype(jnp.bfloat16)
    grads_all = lax.map(feature_grads, (upstream, embeddings))
    flat_grads = grads_all.reshape(micro_count * sample_rows, features, emb_width)
    flat_ids = row_ids.reshape(micro_count * sample_rows, features)

    def one_table(feature_index):
        column = lax.dynamic_index_in_dim(flat_grads, feature_index, 1, False).astype(jnp.float32)
        row_index = lax.dynamic_index_in_dim(flat_ids, feature_index, 1, False)
        return jax.ops.segment_sum(column, row_index, num_segments=ROWS)
    tables = lax.map(one_table, jnp.arange(features, dtype=jnp.int32))
    table_grad = (tables * grad_scale).reshape(SLOTS, TROWS, emb_width)
    return (weight_grad, table_grad)
```

```python
import math

import jax
import jax.numpy as jnp
from jax import lax
from jax.sharding import PartitionSpec as P

TROWS = 512
STRANDS = 2


def passed_along(x, axis, by):
    count = lax.axis_size(axis)
    pairs = [(i, i + by) for i in range(count) if 0 <= i + by < count]
    return lax.ppermute(x, axis, pairs)


def swapped_with(x, axis, flip):
    count = lax.axis_size(axis)
    return lax.ppermute(x, axis, [(i, i ^ flip) for i in range(count)])


def handed_out(passed, axis, position, first, pieces):
    rows = passed.shape[0] // pieces
    total = None
    for j in range(pieces):
        piece = passed[j * rows : (j + 1) * rows]
        if first + j == 0:
            part = jnp.where(position == 0, piece, jnp.zeros_like(piece))
        else:
            part = lax.ppermute(piece, axis, [(0, first + j)])
        total = part if total is None else total + part
    return total


def halved_sum(x, axis, position):
    count = lax.axis_size(axis)
    rows, width = x.shape
    held = x.reshape(count, rows // count, width)
    flip = 1
    while flip < count:
        pairs = held.reshape(held.shape[0] // 2, 2, rows // count, width)
        bit = (position // flip) % 2
        sent = lax.dynamic_index_in_dim(pairs, 1 - bit, 1, False)
        kept = lax.dynamic_index_in_dim(pairs, bit, 1, False)
        got = swapped_with(sent.astype(jnp.bfloat16), axis, flip)
        held = kept + got.astype(jnp.float32)
        flip *= 2
    return held[0]


def direct_sum(x, axis, position):
    count = lax.axis_size(axis)
    rows = x.shape[1] // count
    total = lax.dynamic_slice_in_dim(x, position * rows, rows, 1)
    narrow = x.astype(jnp.bfloat16)
    for flip in range(1, count):
        piece = lax.dynamic_slice_in_dim(narrow, (position ^ flip) * rows, rows, 1)
        total = total + swapped_with(piece, axis, flip).astype(jnp.float32)
    return total


def pair_grads(flat_grad, embedded, features):
    sample_count = flat_grad.shape[0]
    square = flat_grad.reshape(sample_count, features, features)
    direct = jnp.einsum("qfg,qge->qfe", square, embedded, preferred_element_type=jnp.float32)
    swapped = jnp.einsum("qgf,qge->qfe", square, embedded, preferred_element_type=jnp.float32)
    return (direct + swapped).astype(jnp.bfloat16)


def per_device(weights, inputs, preact, cotangent, embeddings, row_ids):
    sections = lax.axis_size("section")
    owners = lax.axis_size("owner")
    section_pos = lax.axis_index("section")
    owner_pos = lax.axis_index("owner")
    micro_count, batch_rows, hidden = cotangent.shape
    features = embeddings.shape[2]
    row_split = max(1, owners // features)
    slot_count = features * row_split // owners
    first_slot = owner_pos * slot_count
    grad_scale = 1.0 / math.sqrt(micro_count * batch_rows * owners)
    layer_w = weights[0]
    layer_in = inputs[0]
    layer_pre = preact[0]
    is_last = section_pos == sections - 1
    quarter = batch_rows // sections
    strand_rows = batch_rows // STRANDS
    strand_pieces = sections // STRANDS

    ids_out = jnp.repeat(
        row_ids.reshape(micro_count * quarter, features), row_split, axis=1
    )
    ids_in = lax.all_to_all(ids_out, "owner", split_axis=1, concat_axis=0, tiled=True)
    ids_in = ids_in.reshape(owners, micro_count, quarter, slot_count)
    slot_ids = first_slot + jnp.arange(slot_count, dtype=jnp.int32)
    ids_in = ids_in - (slot_ids % row_split) * TROWS
    positions = jnp.arange(TROWS, dtype=jnp.int32)

    received = [jnp.zeros((strand_rows, hidden), jnp.bfloat16) for _ in range(STRANDS)]
    slopes = []
    table = None
    moments = micro_count + sections - 1
    for moment in range(moments):
        micro_pos = moment - (sections - 1 - section_pos)
        active = (micro_pos >= 0) & (micro_pos < micro_count)
        clipped = jnp.clip(micro_pos, 0, micro_count - 1)
        portion = None
        for strand in range(STRANDS):
            start = strand * strand_rows
            fresh = cotangent[min(moment, micro_count - 1), start : start + strand_rows]
            incoming = jnp.where(is_last, fresh, received[strand])
            pre_now = lax.dynamic_slice(
                layer_pre, (clipped, start, 0), (1, strand_rows, hidden)
            )[0]
            slope = jnp.where(active & (pre_now > 0), incoming, jnp.zeros_like(incoming))
            slopes.append(slope)
            passed = lax.dot_general(
                slope, layer_w, (((1,), (1,)), ((), ())), preferred_element_type=jnp.float32
            ).astype(jnp.bfloat16)
            if moment + 1 < moments:
                received[strand] = passed_along(passed, "section", -1)
            if moment >= sections - 1:
                part = handed_out(
                    passed, "section", section_pos, strand * strand_pieces, strand_pieces
                )
                portion = part if portion is None else portion + part
        if moment >= sections - 1:
            micro = moment - (sections - 1)
            feat_grads = pair_grads(portion, embeddings[micro], features)
            outgoing = jnp.repeat(feat_grads, row_split, axis=1)
            arrived = lax.all_to_all(
                outgoing, "owner", split_axis=1, concat_axis=0, tiled=True
            )
            places = ids_in[:, micro].reshape(owners * quarter, slot_count)
            onehot = (places[..., None] == positions).astype(jnp.bfloat16)
            rows = jnp.einsum(
                "qsr,qse->sre", onehot, arrived, preferred_element_type=jnp.float32
            )
            table = rows if table is None else table + rows
    table_grad = direct_sum(table, "section", section_pos) * grad_scale
    slope_stack = jnp.stack(slopes).reshape(moments, batch_rows, hidden)
    own_slopes = lax.dynamic_slice_in_dim(
        slope_stack, sections - 1 - section_pos, micro_count, 0
    )
    flat_in = layer_in.reshape(micro_count * batch_rows, hidden)
    flat_slope = own_slopes.reshape(micro_count * batch_rows, hidden)
    partial_grad = lax.dot_general(
        flat_in, flat_slope, (((0,), (0,)), ((), ())), preferred_element_type=jnp.float32
    )
    weight_grad = halved_sum(partial_grad, "owner", owner_pos) * grad_scale
    return (weight_grad[None], table_grad)


def solution(mesh):
    return jax.shard_map(
        per_device,
        mesh=mesh,
        in_specs=(
            P("section", None, None),
            P("section", None, "owner", None),
            P("section", None, "owner", None),
            P(None, "owner", None),
            P(None, ("owner", "section"), None, None),
            P(None, ("owner", "section"), None),
        ),
        out_specs=(P("section", "owner", None), P("owner", "section", None)),
        check_vma=False,
    )
```

```python
import functools
import math

import jax
import jax.numpy as jnp
from jax import lax
from jax.experimental import pallas as pl
from jax.experimental.pallas import tpu as pltpu
from jax.sharding import PartitionSpec as P

TROWS = 512


def swapped_with(x, axis, flip):
    count = lax.axis_size(axis)
    return lax.ppermute(x, axis, [(i, i ^ flip) for i in range(count)])


def halved_sum(x, axis, position):
    count = lax.axis_size(axis)
    rows, width = x.shape
    held = x.reshape(count, rows // count, width)
    flip = 1
    while flip < count:
        pairs = held.reshape(held.shape[0] // 2, 2, rows // count, width)
        bit = (position // flip) % 2
        sent = lax.dynamic_index_in_dim(pairs, 1 - bit, 1, False)
        kept = lax.dynamic_index_in_dim(pairs, bit, 1, False)
        got = swapped_with(sent.astype(jnp.bfloat16), axis, flip)
        held = kept + got.astype(jnp.float32)
        flip *= 2
    return held[0]


def direct_sum(x, axis, position):
    count = lax.axis_size(axis)
    rows = x.shape[1] // count
    total = lax.dynamic_slice_in_dim(x, position * rows, rows, 1)
    narrow = x.astype(jnp.bfloat16)
    for flip in range(1, count):
        piece = lax.dynamic_slice_in_dim(narrow, (position ^ flip) * rows, rows, 1)
        total = total + swapped_with(piece, axis, flip).astype(jnp.float32)
    return total


def chain_kernel(
    dims, w_ref, pre_ref, cot_ref, emb_ref, slope_ref, arrived_ref,
    in_buf, out_buf, portion, square, pairs, outgoing,
    out_sem, in_sem, portion_sem, send_sem, recv_sem, local_sem,
):
    sections, owners, micro_count, quarter, features, width, slots, row_split = dims
    section = lax.axis_index("section")
    owner = lax.axis_index("owner")
    last = sections - 1
    lane_groups = 128 // features

    def along(c):
        return pltpu.make_async_remote_copy(
            src_ref=out_buf.at[c], dst_ref=in_buf.at[c],
            send_sem=out_sem.at[c], recv_sem=in_sem.at[c],
            device_id={"section": lax.rem(section + last, sections)},
            device_id_type=pl.DeviceIdType.MESH,
        )

    def hand(c, m, target):
        return pltpu.make_async_remote_copy(
            src_ref=out_buf.at[c], dst_ref=portion.at[m],
            send_sem=out_sem.at[c], recv_sem=portion_sem.at[m],
            device_id={"section": target},
            device_id_type=pl.DeviceIdType.MESH,
        )

    def exchange(m, target):
        return pltpu.make_async_remote_copy(
            src_ref=outgoing.at[target, m], dst_ref=arrived_ref.at[owner, m],
            send_sem=send_sem.at[target], recv_sem=recv_sem.at[owner],
            device_id={"owner": target},
            device_id_type=pl.DeviceIdType.MESH,
        )

    def chain(m):
        def one(j, carry):
            c = m * sections + j
            rows = pl.ds(pl.multiple_of(j * quarter, quarter), quarter)
            positive = pre_ref[m, rows, :].astype(jnp.float32) > 0

            def masked(incoming):
                grad = incoming.astype(jnp.float32)
                slope_ref[m, rows, :] = jnp.where(positive, grad, 0.0).astype(jnp.bfloat16)

            @pl.when(section == last)
            def _():
                masked(cot_ref[m, rows, :])

            @pl.when(section < last)
            def _():
                along(c).wait_recv()
                masked(in_buf[c])

            out_buf[c] = lax.dot_general(
                slope_ref[m, rows, :], w_ref[...], (((1,), (1,)), ((), ())),
                preferred_element_type=jnp.float32,
            ).astype(jnp.bfloat16)

            @pl.when(section > 0)
            def _():
                along(c).start()

            @pl.when((section == 0) & (j > 0))
            def _():
                hand(c, m, j).start()

            @pl.when((section == 0) & (j == 0))
            def _():
                portion[m] = out_buf[c]

            return carry

        lax.fori_loop(0, sections, one, 0)

    def pair(m):
        @pl.when(section > 0)
        def _():
            hand(0, m, 0).wait_recv()

        for f in range(features):
            group, part = f // lane_groups, f % lane_groups
            block = portion[m, :, group * 128 : (group + 1) * 128].astype(jnp.float32)
            if part:
                block = pltpu.roll(block, 128 - part * features, 1)
            square[pl.ds(f, quarter, stride=features), :] = block
        whole = square[...].reshape(quarter, features, 128)[:, :, :features]
        both = (whole + jnp.swapaxes(whole, 1, 2)).astype(jnp.bfloat16)
        pairs[...] = lax.dot_general(
            both, emb_ref[m], (((2,), (1,)), ((0,), (0,))),
            preferred_element_type=jnp.float32,
        ).reshape(quarter * features, width)
        for target in range(owners):
            for slot in range(slots):
                f = (target * slots + slot) // row_split
                outgoing[target, m, :, slot * width : (slot + 1) * width] = pairs[
                    pl.ds(f, quarter, stride=features), :
                ].astype(jnp.bfloat16)

        def send(k, carry):
            exchange(m, lax.rem(owner + k, owners)).start()
            return carry

        lax.fori_loop(1, owners, send, 0)
        pltpu.make_async_copy(
            outgoing.at[owner, m], arrived_ref.at[owner, m], local_sem.at[m]
        ).start()

    lag = (section + 1) // 2

    def step(t, carry):
        @pl.when(t < micro_count)
        def _():
            chain(t)

        @pl.when((t >= lag) & (t < micro_count + lag))
        def _():
            pair(t - lag)

        return carry

    lax.fori_loop(0, micro_count + sections // 2, step, 0)

    def drain_chain(c, carry):
        @pl.when((section > 0) | (lax.rem(c, sections) > 0))
        def _():
            along(c).wait_send()

        return carry

    lax.fori_loop(0, micro_count * sections, drain_chain, 0)

    def drain_exchange(k, carry):
        target = lax.rem(owner + k, owners)
        everything = pltpu.make_async_remote_copy(
            src_ref=outgoing.at[target], dst_ref=arrived_ref.at[target],
            send_sem=send_sem.at[target], recv_sem=recv_sem.at[target],
            device_id={"owner": target},
            device_id_type=pl.DeviceIdType.MESH,
        )
        everything.wait_send()
        everything.wait_recv()
        return carry

    lax.fori_loop(1, owners, drain_exchange, 0)
    for m in range(micro_count):
        pltpu.make_async_copy(
            outgoing.at[owner, m], arrived_ref.at[owner, m], local_sem.at[m]
        ).wait()


def chain_and_exchange(layer_w, layer_pre, cotangent, embeddings, slots, row_split):
    sections = lax.axis_size("section")
    owners = lax.axis_size("owner")
    micro_count, batch_rows, hidden = cotangent.shape
    quarter, features, width = embeddings.shape[1:]
    chunks = micro_count * sections
    dims = (sections, owners, micro_count, quarter, features, width, slots, row_split)
    vmem = pl.BlockSpec(memory_space=pltpu.VMEM)
    exchanged = (owners, micro_count, quarter, slots * width)
    return pl.pallas_call(
        functools.partial(chain_kernel, dims),
        out_shape=(
            jax.ShapeDtypeStruct(cotangent.shape, jnp.bfloat16),
            jax.ShapeDtypeStruct(exchanged, jnp.bfloat16),
        ),
        in_specs=[vmem] * 4,
        out_specs=(vmem, vmem),
        scratch_shapes=[
            pltpu.VMEM((chunks, quarter, hidden), jnp.bfloat16),
            pltpu.VMEM((chunks, quarter, hidden), jnp.bfloat16),
            pltpu.VMEM((micro_count, quarter, hidden), jnp.bfloat16),
            pltpu.VMEM((quarter * features, 128), jnp.float32),
            pltpu.VMEM((quarter * features, width), jnp.float32),
            pltpu.VMEM(exchanged, jnp.bfloat16),
            pltpu.SemaphoreType.DMA((chunks,)),
            pltpu.SemaphoreType.DMA((chunks,)),
            pltpu.SemaphoreType.DMA((micro_count,)),
            pltpu.SemaphoreType.DMA((owners,)),
            pltpu.SemaphoreType.DMA((owners,)),
            pltpu.SemaphoreType.DMA((micro_count,)),
        ],
        compiler_params=pltpu.CompilerParams(
            has_side_effects=True, vmem_limit_bytes=48 * 1024 * 1024
        ),
    )(layer_w, layer_pre, cotangent, embeddings)


def per_device(weights, inputs, preact, cotangent, embeddings, row_ids):
    owners = lax.axis_size("owner")
    section_pos = lax.axis_index("section")
    owner_pos = lax.axis_index("owner")
    micro_count, batch_rows, hidden = cotangent.shape
    quarter, features, width = embeddings.shape[1:]
    row_split = max(1, owners // features)
    slots = features * row_split // owners
    grad_scale = 1.0 / math.sqrt(micro_count * batch_rows * owners)

    ids_out = jnp.repeat(
        row_ids.reshape(micro_count * quarter, features), row_split, axis=1
    )
    ids_in = lax.all_to_all(ids_out, "owner", split_axis=1, concat_axis=0, tiled=True)
    slot_ids = owner_pos * slots + jnp.arange(slots, dtype=jnp.int32)
    places = ids_in - (slot_ids % row_split) * TROWS
    positions = jnp.arange(TROWS, dtype=jnp.int32)

    slopes, arrived = chain_and_exchange(
        weights[0], preact[0], cotangent, embeddings, slots, row_split
    )
    flat_in = inputs[0].reshape(micro_count * batch_rows, hidden)
    flat_slope = slopes.reshape(micro_count * batch_rows, hidden)
    partial_grad = lax.dot_general(
        flat_in, flat_slope, (((0,), (0,)), ((), ())), preferred_element_type=jnp.float32
    )
    arrived = arrived.reshape(owners * micro_count * quarter, slots * width)
    tables = []
    for slot in range(slots):
        onehot = (places[:, slot, None] == positions).astype(jnp.bfloat16)
        tables.append(
            lax.dot_general(
                onehot, arrived[:, slot * width : (slot + 1) * width],
                (((0,), (0,)), ((), ())), preferred_element_type=jnp.float32,
            )
        )
    table_grad = direct_sum(jnp.stack(tables), "section", section_pos) * grad_scale
    weight_grad = halved_sum(partial_grad, "owner", owner_pos) * grad_scale
    return (weight_grad[None], table_grad)


def solution(mesh):
    return jax.shard_map(
        per_device,
        mesh=mesh,
        in_specs=(
            P("section", None, None),
            P("section", None, "owner", None),
            P("section", None, "owner", None),
            P(None, "owner", None),
            P(None, ("owner", "section"), None, None),
            P(None, ("owner", "section"), None),
        ),
        out_specs=(P("section", "owner", None), P("owner", "section", None)),
        check_vma=False,
    )
```

```python
import functools
import math

import jax
import jax.numpy as jnp
from jax import lax
from jax.experimental import pallas as pl
from jax.experimental.pallas import tpu as pltpu
from jax.sharding import PartitionSpec as P

TROWS = 512


def swapped_with(x, axis, flip):
    count = lax.axis_size(axis)
    return lax.ppermute(x, axis, [(i, i ^ flip) for i in range(count)])


def halved_sum(x, axis, position):
    count = lax.axis_size(axis)
    rows, width = x.shape
    held = x.reshape(count, rows // count, width)
    flip = 1
    while flip < count:
        pairs = held.reshape(held.shape[0] // 2, 2, rows // count, width)
        bit = (position // flip) % 2
        sent = lax.dynamic_index_in_dim(pairs, 1 - bit, 1, False)
        kept = lax.dynamic_index_in_dim(pairs, bit, 1, False)
        got = swapped_with(sent.astype(jnp.bfloat16), axis, flip)
        held = kept + got.astype(jnp.float32)
        flip *= 2
    return held[0]


def direct_sum(x, axis, position):
    count = lax.axis_size(axis)
    rows = x.shape[1] // count
    total = lax.dynamic_slice_in_dim(x, position * rows, rows, 1)
    narrow = x.astype(jnp.bfloat16)
    for flip in range(1, count):
        piece = lax.dynamic_slice_in_dim(narrow, (position ^ flip) * rows, rows, 1)
        total = total + swapped_with(piece, axis, flip).astype(jnp.float32)
    return total


def chain_kernel(
    dims, w_ref, pre_ref, cot_ref, emb_ref, ids_ref, slope_ref, arrived_ref, places_ref,
    in_buf, out_buf, portion, square, pairs, outgoing,
    out_sem, in_sem, portion_sem, send_sem, recv_sem, local_sem,
    ids_send, ids_recv, ids_local,
):
    sections, owners, micro_count, quarter, features, width, slots, row_split = dims
    section = lax.axis_index("section")
    owner = lax.axis_index("owner")
    last = sections - 1
    lane_groups = 128 // features

    def along(c):
        return pltpu.make_async_remote_copy(
            src_ref=out_buf.at[c], dst_ref=in_buf.at[c],
            send_sem=out_sem.at[c], recv_sem=in_sem.at[c],
            device_id={"section": lax.rem(section + last, sections)},
            device_id_type=pl.DeviceIdType.MESH,
        )

    def hand(c, m, target):
        return pltpu.make_async_remote_copy(
            src_ref=out_buf.at[c], dst_ref=portion.at[m],
            send_sem=out_sem.at[c], recv_sem=portion_sem.at[m],
            device_id={"section": target},
            device_id_type=pl.DeviceIdType.MESH,
        )

    def exchange(m, target):
        return pltpu.make_async_remote_copy(
            src_ref=outgoing.at[target, m], dst_ref=arrived_ref.at[owner, m],
            send_sem=send_sem.at[target], recv_sem=recv_sem.at[owner],
            device_id={"owner": target},
            device_id_type=pl.DeviceIdType.MESH,
        )

    def exchange_ids(target, source):
        return pltpu.make_async_remote_copy(
            src_ref=ids_ref.at[target], dst_ref=places_ref.at[source],
            send_sem=ids_send.at[target], recv_sem=ids_recv.at[source],
            device_id={"owner": target},
            device_id_type=pl.DeviceIdType.MESH,
        )

    own_ids = pltpu.make_async_copy(ids_ref.at[owner], places_ref.at[owner], ids_local)
    own_ids.start()

    def send_ids(k, carry):
        exchange_ids(lax.rem(owner + k, owners), owner).start()
        return carry

    lax.fori_loop(1, owners, send_ids, 0)

    def chain(m):
        def one(j, carry):
            c = m * sections + j
            rows = pl.ds(pl.multiple_of(j * quarter, quarter), quarter)
            positive = pre_ref[m, rows, :].astype(jnp.float32) > 0

            def masked(incoming):
                grad = incoming.astype(jnp.float32)
                slope_ref[m, rows, :] = jnp.where(positive, grad, 0.0).astype(jnp.bfloat16)

            @pl.when(section == last)
            def _():
                masked(cot_ref[m, rows, :])

            @pl.when(section < last)
            def _():
                along(c).wait_recv()
                masked(in_buf[c])

            out_buf[c] = lax.dot_general(
                slope_ref[m, rows, :], w_ref[...], (((1,), (1,)), ((), ())),
                preferred_element_type=jnp.float32,
            ).astype(jnp.bfloat16)

            @pl.when(section > 0)
            def _():
                along(c).start()

            @pl.when((section == 0) & (j > 0))
            def _():
                hand(c, m, j).start()

            @pl.when((section == 0) & (j == 0))
            def _():
                portion[m] = out_buf[c]

            return carry

        lax.fori_loop(0, sections, one, 0)

    def pair(m):
        @pl.when(section > 0)
        def _():
            hand(0, m, 0).wait_recv()

        for f in range(features):
            group, part = f // lane_groups, f % lane_groups
            block = portion[m, :, group * 128 : (group + 1) * 128].astype(jnp.float32)
            if part:
                block = pltpu.roll(block, 128 - part * features, 1)
            square[pl.ds(f, quarter, stride=features), :] = block
        whole = square[...].reshape(quarter, features, 128)[:, :, :features]
        both = (whole + jnp.swapaxes(whole, 1, 2)).astype(jnp.bfloat16)
        pairs[...] = lax.dot_general(
            both, emb_ref[m], (((2,), (1,)), ((0,), (0,))),
            preferred_element_type=jnp.float32,
        ).reshape(quarter * features, width)
        for target in range(owners):
            for slot in range(slots):
                f = (target * slots + slot) // row_split
                outgoing[target, m, :, slot * width : (slot + 1) * width] = pairs[
                    pl.ds(f, quarter, stride=features), :
                ].astype(jnp.bfloat16)

        def send(k, carry):
            exchange(m, lax.rem(owner + k, owners)).start()
            return carry

        lax.fori_loop(1, owners, send, 0)
        pltpu.make_async_copy(
            outgoing.at[owner, m], arrived_ref.at[owner, m], local_sem.at[m]
        ).start()

    lag = (section + 1) // 2

    def step(t, carry):
        @pl.when(t < micro_count)
        def _():
            chain(t)

        @pl.when((t >= lag) & (t < micro_count + lag))
        def _():
            pair(t - lag)

        return carry

    lax.fori_loop(0, micro_count + sections // 2, step, 0)

    def drain_chain(c, carry):
        @pl.when((section > 0) | (lax.rem(c, sections) > 0))
        def _():
            along(c).wait_send()

        return carry

    lax.fori_loop(0, micro_count * sections, drain_chain, 0)

    def drain_exchange(k, carry):
        target = lax.rem(owner + k, owners)
        everything = pltpu.make_async_remote_copy(
            src_ref=outgoing.at[target], dst_ref=arrived_ref.at[target],
            send_sem=send_sem.at[target], recv_sem=recv_sem.at[target],
            device_id={"owner": target},
            device_id_type=pl.DeviceIdType.MESH,
        )
        everything.wait_send()
        everything.wait_recv()
        exchange_ids(target, target).wait_send()
        exchange_ids(target, target).wait_recv()
        return carry

    lax.fori_loop(1, owners, drain_exchange, 0)
    own_ids.wait()
    for m in range(micro_count):
        pltpu.make_async_copy(
            outgoing.at[owner, m], arrived_ref.at[owner, m], local_sem.at[m]
        ).wait()


def chain_and_exchange(layer_w, layer_pre, cotangent, embeddings, ids_out, slots, row_split):
    sections = lax.axis_size("section")
    owners = lax.axis_size("owner")
    micro_count, batch_rows, hidden = cotangent.shape
    quarter, features, width = embeddings.shape[1:]
    chunks = micro_count * sections
    dims = (sections, owners, micro_count, quarter, features, width, slots, row_split)
    vmem = pl.BlockSpec(memory_space=pltpu.VMEM)
    exchanged = (owners, micro_count, quarter, slots * width)
    return pl.pallas_call(
        functools.partial(chain_kernel, dims),
        out_shape=(
            jax.ShapeDtypeStruct(cotangent.shape, jnp.bfloat16),
            jax.ShapeDtypeStruct(exchanged, jnp.bfloat16),
            jax.ShapeDtypeStruct(ids_out.shape, jnp.int32),
        ),
        in_specs=[vmem] * 5,
        out_specs=(vmem, vmem, vmem),
        scratch_shapes=[
            pltpu.VMEM((chunks, quarter, hidden), jnp.bfloat16),
            pltpu.VMEM((chunks, quarter, hidden), jnp.bfloat16),
            pltpu.VMEM((micro_count, quarter, hidden), jnp.bfloat16),
            pltpu.VMEM((quarter * features, 128), jnp.float32),
            pltpu.VMEM((quarter * features, width), jnp.float32),
            pltpu.VMEM(exchanged, jnp.bfloat16),
            pltpu.SemaphoreType.DMA((chunks,)),
            pltpu.SemaphoreType.DMA((chunks,)),
            pltpu.SemaphoreType.DMA((micro_count,)),
            pltpu.SemaphoreType.DMA((owners,)),
            pltpu.SemaphoreType.DMA((owners,)),
            pltpu.SemaphoreType.DMA((micro_count,)),
            pltpu.SemaphoreType.DMA((owners,)),
            pltpu.SemaphoreType.DMA((owners,)),
            pltpu.SemaphoreType.DMA(()),
        ],
        compiler_params=pltpu.CompilerParams(
            has_side_effects=True, vmem_limit_bytes=48 * 1024 * 1024
        ),
    )(layer_w, layer_pre, cotangent, embeddings, ids_out)


def per_device(weights, inputs, preact, cotangent, embeddings, row_ids):
    owners = lax.axis_size("owner")
    section_pos = lax.axis_index("section")
    owner_pos = lax.axis_index("owner")
    micro_count, batch_rows, hidden = cotangent.shape
    quarter, features, width = embeddings.shape[1:]
    row_split = max(1, owners // features)
    slots = features * row_split // owners
    grad_scale = 1.0 / math.sqrt(micro_count * batch_rows * owners)

    ids_out = jnp.repeat(
        row_ids.reshape(micro_count * quarter, features).T, row_split, axis=0
    ).reshape(owners, slots, micro_count * quarter)
    positions = jnp.arange(TROWS, dtype=jnp.int32)

    slopes, arrived, places = chain_and_exchange(
        weights[0], preact[0], cotangent, embeddings, ids_out, slots, row_split
    )
    flat_in = inputs[0].reshape(micro_count * batch_rows, hidden)
    flat_slope = slopes.reshape(micro_count * batch_rows, hidden)
    partial_grad = lax.dot_general(
        flat_in, flat_slope, (((0,), (0,)), ((), ())), preferred_element_type=jnp.float32
    )
    arrived = arrived.reshape(owners * micro_count * quarter, slots * width)
    tables = []
    for slot in range(slots):
        row_block = (owner_pos * slots + slot) % row_split
        local_row = places[:, slot].reshape(1, -1) - row_block * TROWS
        onehot = (positions[:, None] == local_row).astype(jnp.bfloat16)
        tables.append(
            lax.dot_general(
                onehot, arrived[:, slot * width : (slot + 1) * width],
                (((1,), (0,)), ((), ())), preferred_element_type=jnp.float32,
            )
        )
    table_grad = direct_sum(jnp.stack(tables), "section", section_pos) * grad_scale
    weight_grad = halved_sum(partial_grad, "owner", owner_pos) * grad_scale
    return (weight_grad[None], table_grad)


def solution(mesh):
    return jax.shard_map(
        per_device,
        mesh=mesh,
        in_specs=(
            P("section", None, None),
            P("section", None, "owner", None),
            P("section", None, "owner", None),
            P(None, "owner", None),
            P(None, ("owner", "section"), None, None),
            P(None, ("owner", "section"), None),
        ),
        out_specs=(P("section", "owner", None), P("owner", "section", None)),
        check_vma=False,
    )
```
